32 devices in a mesh: res: 8 (over z, y), seq: 4 (over x, core).
Axes of the slice: x: 2, y: 2, z: 4, core: 2. Of those that a mesh axis runs over, the one named last changes fastest.
Arguments:
- alignment: bfloat16 [384, 256, 256], P('seq', 'res'), may hold values from -6 to 6
- query_weight: bfloat16 [256, 256], replicated, may hold values from -1 to 1
- w_keyval: bfloat16 [256, 512], replicated, may hold values from -0.375 to 0.375
- w_gate: bfloat16 [256, 256], replicated, may hold values from -0.375 to 0.375
- output_weight: bfloat16 [256, 256], replicated, may hold values from -0.75 to 0.75
- w_factors: bfloat16 [256, 64], replicated, may hold values from -1.5 to 1.5
- w_pair_out: bfloat16 [1024, 128], replicated, may hold values from -0.1875 to 0.1875
Outputs:
- alignment_update: bfloat16 [384, 256, 256], P('seq', 'res')
- pair_representation_update: bfloat16 [256, 256, 128], P(('res', 'seq'))
The draws below stay inside these ranges and needn't reach their ends.
All inputs are finite; a program needn't handle non-finite values.
Results may differ from the reference program's by a relative error of at most 0.012.
The reference program's roundings to bfloat16 on the way count: a program that leaves them out, or rounds other values in their place, can miss the bound.
Values may be sent and summed in bfloat16 or wider, within the bound.
A program may use at most 256 MiB of HBM per device.

```python
import math
import jax
import jax.numpy as jnp
from jax import lax

D = 256
P_SIZE = 128
HEADS = 8
HC = 32
C = 32
HD = 256
S = 384
R = 256


def levels(own_key, dims, pieces, low, largest):
    gain, own = 1.0, jax.random.fold_in(own_key, 6)
    for position, shards_of in pieces:
        draws = jnp.exp(jax.random.uniform(jax.random.fold_in(own, position), (shards_of,), jnp.float32, low / len(pieces), largest / len(pieces)))
        gain = gain * jnp.repeat(draws, dims[position] // shards_of).reshape([-1 if axis == position else 1 for axis in range(len(dims))])
    return gain


def bell_draw(rng, shape, deviation, bound, pieces=(), held_as=jnp.bfloat16):
    drawn = deviation * jax.random.normal(rng, shape, jnp.float32)
    if pieces:
        drawn = drawn * levels(rng, shape, pieces, -0.22, 0.18)
    return jnp.clip(drawn, -bound, bound).astype(held_as)


def setup_inputs(seed: int = 0) -> dict:
    key_list = jax.random.split(jax.random.key(seed), 8)
    return {
        "alignment": bell_draw(key_list[0], (S, R, D), 1.0, 6.0, ((0, 4), (1, 8))),
        "query_weight": bell_draw(key_list[1], (D, HD), (D // 9) ** -0.5, 1.0),
        "w_keyval": bell_draw(key_list[2], (D, 2 * HD), D ** -0.5, 0.375),
        "w_gate": bell_draw(key_list[3], (D, HD), D ** -0.5, 0.375),
        "output_weight": bell_draw(key_list[4], (HD, D), (HD // 4) ** -0.5, 0.75),
        "w_factors": bell_draw(key_list[5], (D, 2 * C), (D // 16) ** -0.5, 1.5),
        "w_pair_out": bell_draw(key_list[6], (C * C, P_SIZE), (C * C) ** -0.5, 0.1875),
    }


def normalize(alignment):
    values = alignment.astype(jnp.float32)
    centered = values - lax.optimization_barrier(jnp.mean(values, axis=-1, keepdims=True))
    spread = lax.optimization_barrier(jnp.mean(centered * centered, axis=-1, keepdims=True))
    return (centered * lax.rsqrt(spread + 1e-05)).astype(jnp.bfloat16)

def reference(alignment, query_weight, w_keyval, w_gate, output_weight, w_factors, w_pair_out):
    normed = normalize(alignment)
    queries = jnp.dot(normed, query_weight, preferred_element_type=jnp.float32).astype(jnp.bfloat16)
    keyvals = jnp.dot(normed, w_keyval, preferred_element_type=jnp.float32).astype(jnp.bfloat16)
    gating = jax.nn.sigmoid(jnp.dot(normed, w_gate, preferred_element_type=jnp.float32))
    hidden = HEADS * HC
    seq_total = normed.shape[0]
    residues = normed.shape[1]
    group_size = math.gcd(residues, 8)

    def attend_block(block_index):
        start_row = (block_index * group_size).astype(jnp.int32)
        query_block = lax.dynamic_slice_in_dim(queries, start_row, group_size, 1).astype(jnp.float32)
        keyval_block = lax.dynamic_slice_in_dim(keyvals, start_row, group_size, 1).astype(jnp.float32)
        per_head_query = query_block.reshape(seq_total, group_size, HEADS, HC)
        head_keys = keyval_block[:, :, :hidden].reshape(seq_total, group_size, HEADS, HC)
        head_values = keyval_block[:, :, hidden:].reshape(seq_total, group_size, HEADS, HC)
        scores = jnp.einsum('qrhd,krhd->rhqk', per_head_query, head_keys) / math.sqrt(HC)
        exponent = jnp.exp(scores)
        weights = exponent.astype(jnp.bfloat16).astype(jnp.float32)
        denominators = jnp.transpose(lax.optimization_barrier(jnp.sum(exponent, axis=-1)), (2, 0, 1))
        weighted = jnp.einsum('rhqk,krhd->qrhd', weights, head_values)
        return (weighted / denominators[:, :, :, None]).reshape(seq_total, group_size, hidden)
    blocks = lax.map(attend_block, jnp.arange(residues // group_size, dtype=jnp.int32))
    attended = jnp.transpose(blocks, (1, 0, 2, 3)).reshape(seq_total, residues, hidden)
    gated_output_rows = (gating * attended).astype(jnp.bfloat16)
    alignment_update = jnp.dot(gated_output_rows, output_weight, preferred_element_type=jnp.float32).astype(jnp.bfloat16)
    factors = jnp.dot(normed, w_factors, preferred_element_type=jnp.float32).astype(jnp.bfloat16)
    factor = factors.shape[2] // 2
    left_factor = factors[:, :, :factor].astype(jnp.float32).reshape(seq_total, residues * factor)
    right_factor = factors[:, :, factor:].astype(jnp.float32).reshape(seq_total, residues * factor)
    channels = w_pair_out.shape[1]
    pair_weight = w_pair_out.astype(jnp.float32).reshape(factor, factor, channels)
    row_block = math.gcd(residues, 32)

    def pair_block(block_index):
        start_col = (block_index * row_block * factor).astype(jnp.int32)
        left_rows = lax.dynamic_slice_in_dim(left_factor, start_col, row_block * factor, 1)
        products = lax.dot_general(left_rows, right_factor, (((0,), (0,)), ((), ())), precision=lax.Precision.HIGHEST, preferred_element_type=jnp.float32)
        products = (products * (1.0 / seq_total)).reshape(row_block, factor, residues, factor)
        return jnp.einsum('icje,cep->ijp', products, pair_weight, precision=lax.Precision.HIGHEST)
    pair_blocks = lax.map(pair_block, jnp.arange(residues // row_block, dtype=jnp.int32))
    pair_representation_update = pair_blocks.reshape(residues, residues, channels).astype(jnp.bfloat16)
    return (alignment_update, pair_representation_update)
```

```python
import functools
import math

import jax
import jax.numpy as jnp
from jax import lax
from jax.experimental import pallas as pl
from jax.experimental.pallas import tpu as pltpu
from jax.sharding import PartitionSpec as P

HEADS = 8
HC = 32
LOG2E = 1.4426950408889634
epsilon = 1e-05
NT = (((1,), (1,)), ((), ()))


def mm(a, b):
    return jnp.dot(a, b, preferred_element_type=jnp.float32)


def mm_nt(a, b):
    return lax.dot_general(a, b, NT, preferred_element_type=jnp.float32)


MESH = pl.DeviceIdType.MESH
COUNT = 2
WIDE = 256


SCALE = LOG2E / math.sqrt(HC)


def chunk_heads(chunk, seqs, wide):
    first = chunk * wide // seqs
    last = ((chunk + 1) * wide - 1) // seqs + 1
    return first, min(last, HEADS)


def prepare_keys(everything, wkv, keys):
    hidden = HEADS * HC
    keys[...] = mm(everything, wkv[:, :hidden]).astype(jnp.bfloat16)


def prepare_values(everything, wkv, values):
    hidden = HEADS * HC
    values[...] = lax.dot_general(
        wkv[:, hidden:], everything, (((0,), (1,)), ((), ())), preferred_element_type=jnp.float32
    ).astype(jnp.bfloat16)


def prepare_queries(own, wq, wg, stacked, gates):
    seqs = own.shape[0]
    hidden = HEADS * HC
    q = mm(own, wq[...]).astype(jnp.bfloat16).astype(jnp.float32)
    head_of = lax.broadcasted_iota(jnp.int32, (seqs, hidden), 1) // HC
    for h in range(HEADS):
        stacked[h * seqs : (h + 1) * seqs, :] = jnp.where(head_of == h, q, 0.0).astype(jnp.bfloat16)
    gates[...] = jax.nn.sigmoid(mm(own, wg[...]))


def score(keys, stacked, chunk, wide):
    rows = stacked[chunk * wide : (chunk + 1) * wide]
    exponent = jnp.exp2(mm_nt(keys[...], rows) * SCALE)
    return exponent.astype(jnp.bfloat16), 1.0 / jnp.sum(exponent, axis=0, keepdims=True)


def weigh(values, attended, chunk, wide, seqs, weights, inverse):
    first, last = chunk_heads(chunk, seqs, wide)
    mixed = mm(values[first * HC : last * HC], weights) * inverse
    for h in range(first, last):
        low, high = max(h * seqs, chunk * wide), min((h + 1) * seqs, (chunk + 1) * wide)
        attended[h * HC : (h + 1) * HC, low - h * seqs : high - h * seqs] = mixed[
            (h - first) * HC : (h - first + 1) * HC, low - chunk * wide : high - chunk * wide
        ]


def finish_residue(attended, gates, wout):
    seqs = gates.shape[0]
    return mm((gates[...] * attended[...].T[:seqs]).astype(jnp.bfloat16), wout[...])


def block_kernel(
    scaling,
    blocks,
    groups,
    x_ref,
    wq_ref,
    wkv_ref,
    wg_ref,
    wout_ref,
    wf_ref,
    wp_ref,
    o_ref,
    pair_ref,
    gathered,
    strided,
    pair_rows,
    spread,
    left_all,
    right_all,
    products,
    outer,
    outgoing,
    incoming,
    cross_send,
    cross_recv,
    twin_send,
    twin_recv,
    relay_send,
    relay_recv,
    ring_send,
    ring_recv,
    share_send,
    share_recv,
    swap_send,
    swap_recv,
    *stages,
):
    seqs, residues, width = x_ref.shape
    depth = seqs * groups
    factor = wf_ref.shape[0] // 2
    pack = 128 // factor
    own_rows = residues // groups
    channels = pair_ref.shape[2]
    half = residues // 2
    parts = residues // COUNT
    half_parts = parts // 2
    hops = blocks // 2
    r = lax.axis_index("res")
    q = lax.axis_index("seq")
    core = lax.rem(q, 2)
    side = q // 2
    twin = q + 1 - 2 * core
    across = lax.rem(q + 2, groups)
    twin_across = lax.rem(twin + 2, groups)

    def ring_of(block):
        z, y = block // 2, lax.rem(block, 2)
        return jnp.where(y == 0, z, blocks - 1 - z)

    def block_of(place):
        return jnp.where(place < blocks // 2, 2 * place, 2 * (blocks - 1 - place) + 1)

    place = ring_of(r)
    ahead = block_of(lax.rem(place + 1, blocks))
    behind = block_of(lax.rem(place + blocks - 1, blocks))

    barrier = pltpu.get_barrier_semaphore()
    for target in ((r, twin), (r, across), (ahead, q), (behind, q)):
        pl.semaphore_signal(barrier, inc=1, device_id=target, device_id_type=MESH)
    pl.semaphore_wait(barrier, 4)

    def part_at(p):
        return lax.rem(p + side * half_parts, parts)

    def rows_of(owner, part):
        return gathered.at[owner, pl.ds(part * COUNT, COUNT)]

    def send(ref, dst, send_sem, recv_sem, target):
        return pltpu.make_async_remote_copy(
            src_ref=ref,
            dst_ref=dst,
            send_sem=send_sem,
            recv_sem=recv_sem,
            device_id=target,
            device_id_type=MESH,
        )

    def cross(owner, p, part):
        block = rows_of(owner, part)
        return send(block, block, cross_send.at[p], cross_recv.at[p], (r, across))

    def direct(owner, p, part):
        block = rows_of(owner, part)
        return send(block, block, twin_send.at[p], twin_recv.at[p], (r, twin))

    def relay(owner, p, part):
        block = rows_of(owner, part)
        return send(block, block, relay_send.at[p], relay_recv.at[p], (r, twin))

    step = 8
    for turn in range(2):
        which = (1 - side) if turn == 0 else side
        base = pl.multiple_of(which * half, half)

        def norm(i, carry):
            values = (
                x_ref[pl.ds(i * step, step), pl.ds(base, half), :]
                .reshape(step * half, width)
                .astype(jnp.float32)
            )
            centered = values - jnp.mean(values, axis=-1, keepdims=True)
            spread = jnp.mean(centered * centered, axis=-1, keepdims=True)
            normed = centered * lax.rsqrt(spread + epsilon)
            for part in range(width // 128):
                strided[part, pl.ds(i * (step * half), step * half), :] = normed[
                    :, part * 128 : (part + 1) * 128
                ]
            return carry

        lax.fori_loop(0, seqs // step, norm, 0)

        def move(k, carry):
            for n in range(COUNT):
                for part in range(width // 128):
                    gathered[q, base + k * COUNT + n, :, part * 128 : (part + 1) * 128] = strided[
                        part, pl.ds(k * COUNT + n, seqs, half), :
                    ].astype(jnp.bfloat16)
            return carry

        def start_across(k, carry):
            cross(q, turn * half_parts + k, which * half_parts + k).start()
            return carry

        def move_and_start(k, carry):
            move(k, carry)
            return start_across(k, carry)

        lax.fori_loop(0, half_parts, move_and_start, 0)

    def start_twin(p, carry):
        direct(q, p, part_at(p)).start()
        return carry

    lax.fori_loop(0, parts, start_twin, 0)

    pair_rows[...] = wp_ref[...].astype(jnp.float32)
    spread[...] = jnp.zeros_like(spread)
    for e in range(factor):
        rows = pair_rows[pl.ds(e, factor, factor), :].astype(jnp.bfloat16)
        for k in range(pack):
            start = (e * pack + k) * factor
            spread[start : start + factor, k * channels : (k + 1) * channels] = rows

    share = COUNT // 2

    def mine(sub):
        return pl.ds(sub * COUNT + core * share, share)

    def twins(sub):
        return pl.ds(sub * COUNT + (1 - core) * share, share)

    def ring_copy(way, sub, hop):
        shift = blocks - hop if way == 0 else hop
        block = block_of(lax.rem(place + shift, blocks))
        ref = right_all.at[block, mine(sub)]
        return send(
            ref,
            ref,
            ring_send.at[way, sub, hop],
            ring_recv.at[way, sub, hop],
            ((ahead if way == 0 else behind), q),
        )

    def landed(way, hop):
        shift = blocks - hop - 1 if way == 0 else hop + 1
        return block_of(lax.rem(place + shift, blocks))

    def arrive(way, sub, hop):
        ref = right_all.at[landed(way, hop), mine(sub)]
        send(
            ref,
            ref,
            ring_send.at[way, sub, hop],
            ring_recv.at[way, sub, hop],
            ((ahead if way == 0 else behind), q),
        ).wait_recv()

    def share_copy(way, sub, hop, outward=True):
        ref = right_all.at[landed(way, hop), mine(sub) if outward else twins(sub)]
        return send(
            ref, ref, share_send.at[way, sub, hop], share_recv.at[way, sub, hop], (r, twin)
        )

    ways = (hops, blocks - 1 - hops)

    def advance(sub, hop):
        for way in range(2):

            @pl.when((hop > 0) & (hop <= ways[way]))
            def _():
                arrive(way, sub, hop - 1)

            @pl.when((hop >= 0) & (hop < ways[way]))
            def _():
                ring_copy(way, sub, hop).start()

            @pl.when((hop > 0) & (hop <= ways[way]))
            def _():
                share_copy(way, sub, hop - 1).start()

    def advance_all(p):
        for sub in range(half_parts):
            advance(sub, p - sub)

    def take_across(p):
        cross(across, p, part_at(p)).wait_recv()
        relay(across, p, part_at(p)).start()

    take_across(0)

    slots = (stages[: len(stages) // 2], stages[len(stages) // 2 :])
    chunks = HEADS * seqs // WIDE

    def residue_at(p, n):
        return part_at(lax.rem(p + parts + n // COUNT, parts)) * COUNT + n % COUNT

    def weigh_last(slot):
        weigh(
            slot[1], slot[4], chunks - 1, WIDE, seqs, slot[5][...], slot[6][0:1, :]
        )

    def emit(slot, residue):
        update = finish_residue(slot[4], slot[3], wout_ref)
        for piece in range(width // 128):
            strided[piece, pl.ds(residue, seqs, residues), :] = update[
                :, piece * 128 : (piece + 1) * 128
            ]

    def attend(slot, other, fresh, emitted):
        everything = gathered[:, fresh].reshape(depth, width) if fresh is not None else None
        held = [score(slot[0], slot[2], 0, WIDE)]
        weigh_last(other)
        for c in range(1, chunks):
            now = score(slot[0], slot[2], c, WIDE)
            if c == chunks - 1:
                slot[5][...], slot[6][0:1, :] = now
            if c == 1:
                emit(other, emitted)
                if fresh is not None:
                    prepare_queries(gathered[q, fresh], wq_ref, wg_ref, other[2], other[3])
            held.append(now)
            weigh(slot[1], slot[4], c - 1, WIDE, seqs, *held[c - 1])
            if c == 1 and fresh is not None:
                prepare_keys(everything, wkv_ref, other[0])
        if fresh is not None:
            prepare_values(everything, wkv_ref, other[1])

    def one_part(p, carry):
        part = part_at(p)
        direct(twin, p, part).wait_recv()
        relay(twin_across, p, part).wait_recv()
        everything = gathered[:, pl.ds(part * COUNT, COUNT)]
        for n in range(COUNT):
            both = mm_nt(wf_ref[...], everything[:, n].reshape(depth, width)).astype(jnp.bfloat16)
            left_all[part * COUNT + n] = both[:factor]

            @pl.when(p < half_parts)
            def _():
                right_all[r, p * COUNT + n] = both[factor:]

        for n in range(COUNT):
            attend(
                slots[(n + 1) % 2], slots[n % 2], residue_at(p, n), residue_at(p, n - 2)
            )
            if n == 0:

                @pl.when(p + 1 < parts)
                def _():
                    take_across(p + 1)

        advance_all(p)
        return carry

    lax.fori_loop(0, parts, one_part, 0)
    attend(slots[1], slots[0], None, residue_at(parts - 1, COUNT - 2))
    weigh_last(slots[1])
    emit(slots[1], residue_at(parts - 1, COUNT - 1))

    def late(p, carry):
        advance_all(p)
        return carry

    lax.fori_loop(parts, half_parts + hops, late, 0)

    for way in range(2):
        for sub in range(half_parts):

            def shared(hop, carry):
                share_copy(way, sub, hop, False).wait_recv()
                return carry

            lax.fori_loop(0, ways[way], shared, 0)

    lanes = own_rows * factor
    span = blocks * half

    def pair_of(owner):
        left = left_all[pl.ds(owner * own_rows, own_rows)].reshape(lanes, depth)

        def one_block(b, inner):
            value = mm_nt(right_all[b].reshape(half * factor, depth), left) * scaling
            for g in range(lanes // 128):
                products[g] = value[:, g * 128 : (g + 1) * 128]
            for e in range(factor):
                for g in range(lanes // 128):
                    outer[
                        pl.ds(pl.multiple_of(g * span + b * half, half), half),
                        e * 128 : (e + 1) * 128,
                    ] = products[g, pl.ds(e, half, factor), :].astype(jnp.bfloat16)
            return inner

        lax.fori_loop(0, blocks, one_block, 0)
        return mm(outer[...], spread[...]).astype(jnp.bfloat16)

    def cut(pair, i):
        g, k = i // pack, i % pack
        return pair[g * span : (g + 1) * span, k * channels : (k + 1) * channels]

    def swap_copy():
        return send(outgoing, incoming, swap_send, swap_recv, (r, across))

    pair = pair_of(across)
    for i in range(own_rows):
        outgoing[i] = cut(pair, i)
    swap_copy().start()

    def place_rows(i, which, value):
        for b in range(blocks):
            start = pl.multiple_of(b * residues + which * half, half)
            pair_ref[i, pl.ds(start, half), :] = value[b * half : (b + 1) * half]

    pair = pair_of(q)
    for i in range(own_rows):
        place_rows(i, side, cut(pair, i))

    def finish(i, carry):
        for piece in range(width // 128):
            o_ref[pl.ds(i * step, step), :, piece * 128 : (piece + 1) * 128] = (
                strided[piece, pl.ds(i * (step * residues), step * residues), :]
                .astype(jnp.bfloat16)
                .reshape(step, residues, 128)
            )
        return carry

    lax.fori_loop(0, seqs // step, finish, 0)
    swap_copy().wait_recv()
    for i in range(own_rows):
        place_rows(i, 1 - side, incoming[i])

    def drain(p, carry):
        cross(q, p, lax.rem(part_at(p) + half_parts, parts)).wait_send()
        direct(q, p, part_at(p)).wait_send()
        relay(across, p, part_at(p)).wait_send()
        return carry

    lax.fori_loop(0, parts, drain, 0)
    for way in range(2):
        for sub in range(half_parts):

            def drain_ring(hop, carry):
                ring_copy(way, sub, hop).wait_send()
                share_copy(way, sub, hop).wait_send()
                return carry

            lax.fori_loop(0, ways[way], drain_ring, 0)
    swap_copy().wait_send()


def per_device(alignment, query_weight, w_keyval, w_gate, output_weight, w_factors, w_pair_out):
    seqs, residues, width = alignment.shape
    groups = lax.axis_size("seq")
    blocks = lax.axis_size("res")
    depth = seqs * groups
    factor = w_factors.shape[1] // 2
    hidden = HEADS * HC
    stage = [
        pltpu.VMEM((depth, hidden), jnp.bfloat16),
        pltpu.VMEM((hidden, depth), jnp.bfloat16),
        pltpu.VMEM((HEADS * seqs, hidden), jnp.bfloat16),
        pltpu.VMEM((seqs, hidden), jnp.float32),
        pltpu.VMEM((hidden, 128), jnp.float32),
        pltpu.VMEM((depth, WIDE), jnp.bfloat16),
        pltpu.VMEM((8, WIDE), jnp.float32),
    ]
    channels = w_pair_out.shape[1]
    own_rows = residues // groups
    half = residues // 2
    parts = residues // COUNT
    hops = blocks // 2
    pack = 128 // factor
    subs = parts // 2
    span = blocks * half
    vmem = pl.BlockSpec(memory_space=pltpu.VMEM)
    dma = pltpu.SemaphoreType.DMA
    return pl.pallas_call(
        functools.partial(block_kernel, 1.0 / depth, blocks, groups),
        in_specs=[vmem] * 7,
        out_specs=[vmem] * 2,
        out_shape=[
            jax.ShapeDtypeStruct((seqs, residues, width), jnp.bfloat16),
            jax.ShapeDtypeStruct((own_rows, blocks * residues, channels), jnp.bfloat16),
        ],
        scratch_shapes=[
            pltpu.VMEM((groups, residues, seqs, width), jnp.bfloat16),
            pltpu.VMEM((width // 128, seqs * residues, 128), jnp.float32),
            pltpu.VMEM((factor * factor, channels), jnp.float32),
            pltpu.VMEM((factor * 128, pack * channels), jnp.bfloat16),
            pltpu.VMEM((residues, factor, depth), jnp.bfloat16),
            pltpu.VMEM((blocks, half, factor, depth), jnp.bfloat16),
            pltpu.VMEM((own_rows // pack, half * factor, 128), jnp.float32),
            pltpu.VMEM((own_rows // pack * span, factor * 128), jnp.bfloat16),
            pltpu.VMEM((own_rows, span, channels), jnp.bfloat16),
            pltpu.VMEM((own_rows, span, channels), jnp.bfloat16),
            dma((parts,)),
            dma((parts,)),
            dma((parts,)),
            dma((parts,)),
            dma((parts,)),
            dma((parts,)),
            dma((2, subs, hops)),
            dma((2, subs, hops)),
            dma((2, subs, hops)),
            dma((2, subs, hops)),
            dma,
            dma,
        ]
        + stage * 2,
        compiler_params=pltpu.CompilerParams(
            vmem_limit_bytes=62 * 1024 * 1024, collective_id=0, has_side_effects=True
        ),
        name="block",
    )(alignment, query_weight, w_keyval, w_gate, output_weight, w_factors.T, w_pair_out)


def solution(mesh):
    in_specs = (P("seq", "res", None), P(), P(), P(), P(), P(), P())
    out_specs = (P("seq", "res", None), P(("res", "seq"), None, None))
    return jax.shard_map(
        per_device, mesh=mesh, in_specs=in_specs, out_specs=out_specs, check_vma=False
    )
```

```python
import functools
import math

import jax
import jax.numpy as jnp
from jax import lax
from jax.experimental import pallas as pl
from jax.experimental.pallas import tpu as pltpu
from jax.sharding import PartitionSpec as P

HEADS = 8
HC = 32
LOG2E = 1.4426950408889634
epsilon = 1e-05
NT = (((1,), (1,)), ((), ()))


def mm(a, b):
    return jnp.dot(a, b, preferred_element_type=jnp.float32)


def mm_nt(a, b):
    return lax.dot_general(a, b, NT, preferred_element_type=jnp.float32)


MESH = pl.DeviceIdType.MESH
COUNT = 2
WIDE = 256
PITCH_PAD = 4
FIRST_EVENT = 3
EARLY_PARTS = 2


SCALE = LOG2E / math.sqrt(HC)


def chunk_heads(chunk, seqs, wide):
    first = chunk * wide // seqs
    last = ((chunk + 1) * wide - 1) // seqs + 1
    return first, min(last, HEADS)


def prepare_keys(everything, wkv, keys):
    hidden = HEADS * HC
    keys[...] = mm(everything, wkv[:, :hidden]).astype(jnp.bfloat16)


def prepare_values(everything, wkv, values):
    hidden = HEADS * HC
    values[...] = lax.dot_general(
        wkv[:, hidden:], everything, (((0,), (1,)), ((), ())), preferred_element_type=jnp.float32
    ).astype(jnp.bfloat16)


def prepare_queries(own, wq, wg, stacked, gates):
    seqs = own.shape[0]
    hidden = HEADS * HC
    q = mm(own, wq[...]).astype(jnp.bfloat16).astype(jnp.float32)
    head_of = lax.broadcasted_iota(jnp.int32, (seqs, hidden), 1) // HC
    for h in range(HEADS):
        stacked[h * seqs : (h + 1) * seqs, :] = jnp.where(head_of == h, q, 0.0).astype(jnp.bfloat16)
    gates[...] = jax.nn.sigmoid(mm(own, wg[...]))


def score(keys, stacked, chunk, wide):
    rows = stacked[chunk * wide : (chunk + 1) * wide]
    exponent = jnp.exp2(mm_nt(keys[...], rows) * SCALE)
    return exponent.astype(jnp.bfloat16), 1.0 / jnp.sum(exponent, axis=0, keepdims=True)


def weigh(values, attended, chunk, wide, seqs, weights, inverse):
    first, last = chunk_heads(chunk, seqs, wide)
    mixed = mm(values[first * HC : last * HC], weights) * inverse
    for h in range(first, last):
        low, high = max(h * seqs, chunk * wide), min((h + 1) * seqs, (chunk + 1) * wide)
        attended[h * HC : (h + 1) * HC, low - h * seqs : high - h * seqs] = mixed[
            (h - first) * HC : (h - first + 1) * HC, low - chunk * wide : high - chunk * wide
        ]


def finish_residue(attended, gates, wout):
    seqs = gates.shape[0]
    return mm((gates[...] * attended[...].T[:seqs]).astype(jnp.bfloat16), wout[...])


def block_kernel(
    scaling,
    blocks,
    groups,
    x_ref,
    wq_ref,
    wkv_ref,
    wg_ref,
    wout_ref,
    wf_ref,
    wp_ref,
    o_ref,
    pair_ref,
    gathered,
    strided,
    pair_rows,
    spread,
    placed,
    left_rows,
    left_all,
    right_all,
    outer,
    products,
    cross_send,
    cross_recv,
    twin_send,
    twin_recv,
    relay_send,
    relay_recv,
    factor_send,
    factor_recv,
    ring_send,
    ring_recv,
    share_send,
    share_recv,
    *stages,
):
    seqs, residues, width = x_ref.shape
    depth = seqs * groups
    factor = wf_ref.shape[0] // 2
    pack = 128 // factor
    own_rows = residues // groups
    channels = pair_ref.shape[2]
    half = residues // 2
    parts = residues // COUNT
    half_parts = parts // 2
    hops = blocks // 2
    pitch = residues + PITCH_PAD
    r = lax.axis_index("res")
    q = lax.axis_index("seq")
    core = lax.rem(q, 2)
    side = q // 2
    twin = q + 1 - 2 * core
    across = lax.rem(q + 2, groups)
    twin_across = lax.rem(twin + 2, groups)

    def ring_of(block):
        z, y = block // 2, lax.rem(block, 2)
        return jnp.where(y == 0, z, blocks - 1 - z)

    def block_of(place):
        return jnp.where(place < blocks // 2, 2 * place, 2 * (blocks - 1 - place) + 1)

    place = ring_of(r)
    ahead = block_of(lax.rem(place + 1, blocks))
    behind = block_of(lax.rem(place + blocks - 1, blocks))

    barrier = pltpu.get_barrier_semaphore()
    for target in ((r, twin), (r, across), (ahead, q), (behind, q)):
        pl.semaphore_signal(barrier, inc=1, device_id=target, device_id_type=MESH)
    pl.semaphore_wait(barrier, 4)

    def part_at(p):
        return lax.rem(p + side * half_parts, parts)

    def rows_of(owner, part):
        return gathered.at[owner, pl.ds(part * COUNT, COUNT)]

    def send(ref, send_sem, recv_sem, target):
        return pltpu.make_async_remote_copy(
            src_ref=ref,
            dst_ref=ref,
            send_sem=send_sem,
            recv_sem=recv_sem,
            device_id=target,
            device_id_type=MESH,
        )

    def cross(owner, p, part):
        return send(rows_of(owner, part), cross_send.at[p], cross_recv.at[p], (r, across))

    def direct(owner, p, part):
        return send(rows_of(owner, part), twin_send.at[p], twin_recv.at[p], (r, twin))

    def relay(owner, p, part):
        return send(rows_of(owner, part), relay_send.at[p], relay_recv.at[p], (r, twin))

    def cross_own(p):
        return cross(q, p, lax.rem(part_at(p) + half_parts, parts))

    step = 8
    for turn in range(2):
        which = (1 - side) if turn == 0 else side
        base = pl.multiple_of(which * half, half)

        def norm(i, carry):
            values = (
                x_ref[pl.ds(i * step, step), pl.ds(base, half), :]
                .reshape(step * half, width)
                .astype(jnp.float32)
            )
            centered = values - jnp.mean(values, axis=-1, keepdims=True)
            variance = jnp.mean(centered * centered, axis=-1, keepdims=True)
            normed = centered * lax.rsqrt(variance + epsilon)
            for part in range(width // 128):
                for k in range(step):
                    strided[part, pl.ds((i * step + k) * pitch, half), :] = normed[
                        k * half : (k + 1) * half, part * 128 : (part + 1) * 128
                    ]
            return carry

        lax.fori_loop(0, seqs // step, norm, 0, unroll=2)

        def move(k, carry):
            for n in range(COUNT):
                for part in range(width // 128):
                    gathered[q, base + k * COUNT + n, :, part * 128 : (part + 1) * 128] = strided[
                        part, pl.ds(k * COUNT + n, seqs, pitch), :
                    ].astype(jnp.bfloat16)
            return carry

        if turn == 0:
            for k in range(EARLY_PARTS):
                move(k, 0)
                cross_own(k).start()
            lax.fori_loop(EARLY_PARTS, half_parts, move, 0, unroll=2)
        else:
            lax.fori_loop(0, half_parts, move, 0, unroll=2)

    def start_twin(p, carry):
        direct(q, p, part_at(p)).start()
        return carry

    lax.fori_loop(0, parts, start_twin, 0)

    row = lax.broadcasted_iota(jnp.int32, (factor, pack * 128), 0)
    lane = lax.broadcasted_iota(jnp.int32, (factor, pack * 128), 1)
    chosen = jnp.where(lax.rem(lane, 128) == (lane // 128) * factor + row, 1.0, 0.0)
    placed[...] = lax.dot_general(
        wf_ref[factor:],
        chosen.astype(jnp.bfloat16),
        (((0,), (0,)), ((), ())),
        preferred_element_type=jnp.float32,
    ).astype(jnp.bfloat16)

    for g in range(residues // pack):
        total = mm(gathered[q, g * pack], placed[:, :128])
        for k in range(1, pack):
            total = total + mm(gathered[q, g * pack + k], placed[:, k * 128 : (k + 1) * 128])
        right_all[r, q, :, g * 128 : (g + 1) * 128] = total.astype(jnp.bfloat16)

    def factor_copy(kind, owner):
        target = (r, across) if kind == 0 else (r, twin)
        return send(right_all.at[r, owner], factor_send.at[kind], factor_recv.at[kind], target)

    def owner_of(piece, own=True):
        if own:
            return jnp.where(piece == 0, q, across)
        return jnp.where(piece == 0, twin, twin_across)

    def shifted(way, hop):
        return block_of(lax.rem(place + (blocks - hop if way == 0 else hop), blocks))

    def neighbour(way):
        return ((ahead if way == 0 else behind), q)

    def ring_copy(way, piece, hop):
        ref = right_all.at[shifted(way, hop), owner_of(piece)]
        sems = (ring_send.at[way, piece, hop], ring_recv.at[way, piece, hop])
        return send(ref, *sems, neighbour(way))

    def arrival(way, piece, hop):
        ref = right_all.at[shifted(way, hop + 1), owner_of(piece)]
        sems = (ring_send.at[way, piece, hop], ring_recv.at[way, piece, hop])
        return send(ref, *sems, neighbour(way))

    def share_copy(way, piece, hop, outward=True):
        ref = right_all.at[shifted(way, hop + 1), owner_of(piece, outward)]
        sems = (share_send.at[way, piece, hop], share_recv.at[way, piece, hop])
        return send(ref, *sems, (r, twin))

    def reach(way, piece):
        return jnp.where(piece == way, hops, hops - 1)

    def event(piece, hop):
        for way in range(2):

            @pl.when(hop < reach(way, piece))
            def _():
                arrival(way, piece, hop).wait_recv()

            @pl.when(hop + 1 < reach(way, piece))
            def _():
                ring_copy(way, piece, hop + 1).start()

            @pl.when(hop < reach(way, piece))
            def _():
                share_copy(way, piece, hop).start()

    factor_copy(0, q).start()
    for way in range(2):
        ring_copy(way, 0, 0).start()
    factor_copy(1, q).start()

    def start_across(p, carry):
        cross_own(p).start()
        return carry

    lax.fori_loop(EARLY_PARTS, parts, start_across, 0)

    def take_factors():
        factor_copy(0, across).wait_recv()
        for way in range(2):
            ring_copy(way, 1, 0).start()
        factor_copy(2, across).start()

    pair_rows[...] = wp_ref[...].astype(jnp.float32)
    spread[...] = jnp.zeros_like(spread)
    for c in range(factor):
        rows = pair_rows[c * factor : (c + 1) * factor, :].astype(jnp.bfloat16)
        for k in range(pack):
            start = (c * pack + k) * factor
            spread[start : start + factor, k * channels : (k + 1) * channels] = rows

    def take_across(p):
        cross(across, p, part_at(p)).wait_recv()
        relay(across, p, part_at(p)).start()

    def make_left():
        for i in range(own_rows):
            rows = gathered[:, q * own_rows + i].reshape(depth, width)
            value = mm_nt(wf_ref[:factor], rows)
            for k in range(depth // 128):
                left_rows[k, pl.ds(i, factor, own_rows), :] = value[:, k * 128 : (k + 1) * 128]
        for k in range(depth // 128):
            left_all[:, k * 128 : (k + 1) * 128] = left_rows[k].astype(jnp.bfloat16)

    jgroups = residues // pack

    def block_at(k):
        last = 2 * hops - 1
        hop = (k - 1) // 2 + 1
        even = jnp.where(lax.rem(k, 2) == 1, blocks - hop, hop)
        shift = jnp.where(k == 0, 0, jnp.where(k == last, hops, even))
        return block_of(lax.rem(place + shift, blocks))

    def pair_wait(k):
        last = 2 * hops - 1

        @pl.when(k == 0)
        def _():
            factor_copy(1, twin).wait_recv()
            factor_copy(2, twin_across).wait_recv()

        for way in range(2):

            @pl.when((k > 0) & (k < last) & (lax.rem(k + 1, 2) == way))
            def _():
                for piece in range(2):
                    share_copy(way, piece, (k - 1) // 2, False).wait_recv()

            @pl.when(k == last)
            def _():
                share_copy(way, way, hops - 1, False).wait_recv()

    def pair_first(k):
        block = block_at(k)
        value = mm(left_all[...], right_all[block].reshape(depth, residues * factor))
        base = pl.multiple_of(lax.rem(k, 2) * (jgroups * own_rows), jgroups * own_rows)
        for c in range(factor):
            for m in range(jgroups // 2):
                outer[
                    pl.ds(base + m * 2 * own_rows, 2 * own_rows), c * 128 : (c + 1) * 128
                ] = jnp.concatenate(
                    [
                        value[c * own_rows : (c + 1) * own_rows, g * 128 : (g + 1) * 128]
                        for g in (2 * m, 2 * m + 1)
                    ],
                    axis=0,
                ).astype(jnp.bfloat16)

    def pair_second(k):
        value = mm(outer[...], spread[...]) * scaling
        for t in range(2):
            for g in range(jgroups):
                start = (t * jgroups + g) * own_rows
                for j in range(pack):
                    products[t, pl.ds(g * pack + j, own_rows, pitch), :] = value[
                        start : start + own_rows, j * channels : (j + 1) * channels
                    ]
        for t in range(2):
            start = pl.multiple_of(block_at(k - 1 + t) * residues, residues)
            for i in range(own_rows):
                pair_ref[i, pl.ds(start, residues), :] = products[
                    t, pl.ds(i * pitch, residues), :
                ].astype(jnp.bfloat16)

    def pair_step(k):
        pair_wait(k)
        pair_first(k)

        @pl.when(lax.rem(k, 2) == 1)
        def _():
            pair_second(k)

    slots = (stages[: len(stages) // 2], stages[len(stages) // 2 :])
    chunks = HEADS * seqs // WIDE

    def residue_at(p, n):
        return part_at(lax.rem(p + parts + n // COUNT, parts)) * COUNT + n % COUNT

    def weigh_last(slot):
        weigh(slot[1], slot[4], chunks - 1, WIDE, seqs, slot[5][...], slot[6][0:1, :])

    def emit(slot, residue):
        update = finish_residue(slot[4], slot[3], wout_ref)
        for piece in range(width // 128):
            strided[piece, pl.ds(residue, seqs, pitch), :] = update[
                :, piece * 128 : (piece + 1) * 128
            ]

    def attend(slot, other, fresh, emitted):
        everything = gathered[:, fresh].reshape(depth, width) if fresh is not None else None
        held = [score(slot[0], slot[2], 0, WIDE)]
        weigh_last(other)
        for c in range(1, chunks):
            now = score(slot[0], slot[2], c, WIDE)
            if c == chunks - 1:
                slot[5][...], slot[6][0:1, :] = now
            if c == 1:
                emit(other, emitted)
                if fresh is not None:
                    prepare_queries(gathered[q, fresh], wq_ref, wg_ref, other[2], other[3])
            held.append(now)
            weigh(slot[1], slot[4], c - 1, WIDE, seqs, *held[c - 1])
            if c == 1 and fresh is not None:
                prepare_keys(everything, wkv_ref, other[0])
        if fresh is not None:
            prepare_values(everything, wkv_ref, other[1])

    take_across(0)
    events = 2 * hops
    loop_events = min((parts - FIRST_EVENT + 1) // 2, events)
    pair_start = half_parts
    loop_pairs = 1
    while (
        pair_start + loop_pairs < parts
        and FIRST_EVENT + 2 * ((loop_pairs - 1) // 2 * 2 + 1) <= pair_start + loop_pairs
    ):
        loop_pairs += 1

    def one_part(p, carry):
        part = part_at(p)

        @pl.when(p + 1 < parts)
        def _():
            take_across(p + 1)

        @pl.when(p == FIRST_EVENT - 1)
        def _():
            take_factors()

        number = p - FIRST_EVENT

        @pl.when((number >= 0) & (lax.rem(number, 2) == 0) & (number // 2 < loop_events))
        def _():
            event(lax.rem(number // 2, 2), number // 4)

        direct(twin, p, part).wait_recv()
        relay(twin_across, p, part).wait_recv()
        for n in range(COUNT):
            attend(slots[(n + 1) % 2], slots[n % 2], residue_at(p, n), residue_at(p, n - 2))

        @pl.when(p == pair_start - 1)
        def _():
            make_left()

        @pl.when((p >= pair_start) & (p - pair_start < loop_pairs))
        def _():
            pair_step(p - pair_start)

        return carry

    lax.fori_loop(0, parts, one_part, 0)

    def late(e, carry):
        event(lax.rem(e, 2), e // 2)
        return carry

    lax.fori_loop(loop_events, events, late, 0)
    attend(slots[1], slots[0], None, residue_at(parts - 1, COUNT - 2))
    weigh_last(slots[1])
    emit(slots[1], residue_at(parts - 1, COUNT - 1))

    def rest(k, carry):
        pair_step(k)
        return carry

    lax.fori_loop(loop_pairs, blocks, rest, 0)

    def finish(i, carry):
        for piece in range(width // 128):
            for k in range(step):
                o_ref[i * step + k, :, piece * 128 : (piece + 1) * 128] = strided[
                    piece, pl.ds((i * step + k) * pitch, residues), :
                ].astype(jnp.bfloat16)
        return carry

    lax.fori_loop(0, seqs // step, finish, 0)

    def drain(p, carry):
        cross_own(p).wait_send()
        direct(q, p, part_at(p)).wait_send()
        relay(across, p, part_at(p)).wait_send()
        return carry

    lax.fori_loop(0, parts, drain, 0)
    for kind, owner in ((0, q), (1, q), (2, across)):
        factor_copy(kind, owner).wait_send()
    for way in range(2):
        for piece in range(2):

            def drain_ring(hop, carry):
                ring_copy(way, piece, hop).wait_send()
                share_copy(way, piece, hop).wait_send()
                return carry

            lax.fori_loop(0, hops if way == piece else hops - 1, drain_ring, 0)


def per_device(alignment, query_weight, w_keyval, w_gate, output_weight, w_factors, w_pair_out):
    seqs, residues, width = alignment.shape
    groups = lax.axis_size("seq")
    blocks = lax.axis_size("res")
    depth = seqs * groups
    factor = w_factors.shape[1] // 2
    hidden = HEADS * HC
    stage = [
        pltpu.VMEM((depth, hidden), jnp.bfloat16),
        pltpu.VMEM((hidden, depth), jnp.bfloat16),
        pltpu.VMEM((HEADS * seqs, hidden), jnp.bfloat16),
        pltpu.VMEM((seqs, hidden), jnp.float32),
        pltpu.VMEM((hidden, 128), jnp.float32),
        pltpu.VMEM((depth, WIDE), jnp.bfloat16),
        pltpu.VMEM((8, WIDE), jnp.float32),
    ]
    channels = w_pair_out.shape[1]
    own_rows = residues // groups
    parts = residues // COUNT
    hops = blocks // 2
    pack = 128 // factor
    pitch = residues + PITCH_PAD
    vmem = pl.BlockSpec(memory_space=pltpu.VMEM)
    dma = pltpu.SemaphoreType.DMA
    return pl.pallas_call(
        functools.partial(block_kernel, 1.0 / depth, blocks, groups),
        in_specs=[vmem] * 7,
        out_specs=[vmem] * 2,
        out_shape=[
            jax.ShapeDtypeStruct((seqs, residues, width), jnp.bfloat16),
            jax.ShapeDtypeStruct((own_rows, blocks * residues, channels), jnp.bfloat16),
        ],
        scratch_shapes=[
            pltpu.VMEM((groups, residues, seqs, width), jnp.bfloat16),
            pltpu.VMEM((width // 128, seqs * pitch, 128), jnp.float32),
            pltpu.VMEM((factor * factor, channels), jnp.float32),
            pltpu.VMEM((factor * 128, pack * channels), jnp.bfloat16),
            pltpu.VMEM((width, pack * 128), jnp.bfloat16),
            pltpu.VMEM((depth // 128, factor * own_rows, 128), jnp.float32),
            pltpu.VMEM((factor * own_rows, depth), jnp.bfloat16),
            pltpu.VMEM((blocks, groups, seqs, residues * factor), jnp.bfloat16),
            pltpu.VMEM((2 * residues // pack * own_rows, factor * 128), jnp.bfloat16),
            pltpu.VMEM((2, own_rows * pitch, channels), jnp.float32),
            dma((parts,)),
            dma((parts,)),
            dma((parts,)),
            dma((parts,)),
            dma((parts,)),
            dma((parts,)),
            dma((3,)),
            dma((3,)),
            dma((2, 2, hops)),
            dma((2, 2, hops)),
            dma((2, 2, hops)),
            dma((2, 2, hops)),
        ]
        + stage * 2,
        compiler_params=pltpu.CompilerParams(
            vmem_limit_bytes=62 * 1024 * 1024, collective_id=0, has_side_effects=True
        ),
        name="block",
    )(alignment, query_weight, w_keyval, w_gate, output_weight, w_factors.T, w_pair_out)


def solution(mesh):
    in_specs = (P("seq", "res", None), P(), P(), P(), P(), P(), P())
    out_specs = (P("seq", "res", None), P(("res", "seq"), None, None))
    return jax.shard_map(
        per_device, mesh=mesh, in_specs=in_specs, out_specs=out_specs, check_vma=False
    )
```

```python
import functools
import math

import jax
import jax.numpy as jnp
from jax import lax
from jax.experimental import pallas as pl
from jax.experimental.pallas import tpu as pltpu
from jax.sharding import PartitionSpec as P

HEADS = 8
HC = 32
LOG2E = 1.4426950408889634
epsilon = 1e-05
NT = (((1,), (1,)), ((), ()))


def mm(a, b):
    return jnp.dot(a, b, preferred_element_type=jnp.float32)


def mm_nt(a, b):
    return lax.dot_general(a, b, NT, preferred_element_type=jnp.float32)


MESH = pl.DeviceIdType.MESH
COUNT = 2
WIDE = 256
PITCH_PAD = 4
FIRST_EVENT = 3
EARLY_PARTS = 2
PIECES = 8


SCALE = LOG2E / math.sqrt(HC)


def chunk_heads(chunk, seqs, wide):
    first = chunk * wide // seqs
    last = ((chunk + 1) * wide - 1) // seqs + 1
    return first, min(last, HEADS)


def prepare_keys(everything, wkv, keys):
    hidden = HEADS * HC
    keys[...] = mm(everything, wkv[:, :hidden]).astype(jnp.bfloat16)


def prepare_values(everything, wkv, values):
    hidden = HEADS * HC
    values[...] = lax.dot_general(
        wkv[:, hidden:], everything, (((0,), (1,)), ((), ())), preferred_element_type=jnp.float32
    ).astype(jnp.bfloat16)


def prepare_queries(own, wq, wg, stacked, gates):
    seqs = own.shape[0]
    hidden = HEADS * HC
    q = mm(own, wq[...]).astype(jnp.bfloat16).astype(jnp.float32)
    head_of = lax.broadcasted_iota(jnp.int32, (seqs, hidden), 1) // HC
    for h in range(HEADS):
        stacked[h * seqs : (h + 1) * seqs, :] = jnp.where(head_of == h, q, 0.0).astype(jnp.bfloat16)
    gates[...] = jax.nn.sigmoid(mm(own, wg[...]))


def score(keys, stacked, chunk, wide):
    rows = stacked[chunk * wide : (chunk + 1) * wide]
    exponent = jnp.exp2(mm_nt(keys[...], rows) * SCALE)
    return exponent.astype(jnp.bfloat16), 1.0 / jnp.sum(exponent, axis=0, keepdims=True)


def weigh(values, attended, chunk, wide, seqs, weights, inverse):
    first, last = chunk_heads(chunk, seqs, wide)
    mixed = mm(values[first * HC : last * HC], weights) * inverse
    for h in range(first, last):
        low, high = max(h * seqs, chunk * wide), min((h + 1) * seqs, (chunk + 1) * wide)
        attended[h * HC : (h + 1) * HC, low - h * seqs : high - h * seqs] = mixed[
            (h - first) * HC : (h - first + 1) * HC, low - chunk * wide : high - chunk * wide
        ]


def finish_residue(attended, gates, wout):
    seqs = gates.shape[0]
    return mm((gates[...] * attended[...].T[:seqs]).astype(jnp.bfloat16), wout[...])


def block_kernel(
    scaling,
    blocks,
    groups,
    x_ref,
    wq_ref,
    wkv_ref,
    wg_ref,
    wout_ref,
    wf_ref,
    wp_ref,
    o_ref,
    pair_ref,
    gathered,
    strided,
    pair_rows,
    spread,
    placed,
    left_rows,
    left_all,
    right_all,
    outer,
    products,
    cross_send,
    cross_recv,
    twin_send,
    twin_recv,
    relay_send,
    relay_recv,
    factor_send,
    factor_recv,
    ring_send,
    ring_recv,
    share_send,
    share_recv,
    *stages,
):
    seqs, residues, width = x_ref.shape
    depth = seqs * groups
    factor = wf_ref.shape[0] // 2
    pack = 128 // factor
    own_rows = residues // groups
    channels = pair_ref.shape[2]
    half = residues // 2
    parts = residues // COUNT
    half_parts = parts // 2
    hops = blocks // 2
    pitch = residues + PITCH_PAD
    r = lax.axis_index("res")
    q = lax.axis_index("seq")
    core = lax.rem(q, 2)
    side = q // 2
    twin = q + 1 - 2 * core
    across = lax.rem(q + 2, groups)
    twin_across = lax.rem(twin + 2, groups)

    def ring_of(block):
        z, y = block // 2, lax.rem(block, 2)
        return jnp.where(y == 0, z, blocks - 1 - z)

    def block_of(place):
        return jnp.where(place < blocks // 2, 2 * place, 2 * (blocks - 1 - place) + 1)

    place = ring_of(r)
    ahead = block_of(lax.rem(place + 1, blocks))
    behind = block_of(lax.rem(place + blocks - 1, blocks))

    barrier = pltpu.get_barrier_semaphore()
    for target in ((r, twin), (r, across), (ahead, q), (behind, q)):
        pl.semaphore_signal(barrier, inc=1, device_id=target, device_id_type=MESH)
    pl.semaphore_wait(barrier, 4)

    def part_at(p):
        return lax.rem(p + side * half_parts, parts)

    def rows_of(owner, part):
        return gathered.at[owner, pl.ds(part * COUNT, COUNT)]

    def send(ref, send_sem, recv_sem, target):
        return pltpu.make_async_remote_copy(
            src_ref=ref,
            dst_ref=ref,
            send_sem=send_sem,
            recv_sem=recv_sem,
            device_id=target,
            device_id_type=MESH,
        )

    def cross(owner, p, part):
        return send(rows_of(owner, part), cross_send.at[p], cross_recv.at[p], (r, across))

    def direct(owner, p, part):
        return send(rows_of(owner, part), twin_send.at[p], twin_recv.at[p], (r, twin))

    def relay(owner, p, part):
        return send(rows_of(owner, part), relay_send.at[p], relay_recv.at[p], (r, twin))

    def cross_own(p):
        return cross(q, p, lax.rem(part_at(p) + half_parts, parts))

    step = 8
    for turn in range(2):
        which = (1 - side) if turn == 0 else side
        base = pl.multiple_of(which * half, half)

        def norm(i, carry):
            values = (
                x_ref[pl.ds(i * step, step), pl.ds(base, half), :]
                .reshape(step * half, width)
                .astype(jnp.float32)
            )
            centered = values - jnp.mean(values, axis=-1, keepdims=True)
            variance = jnp.mean(centered * centered, axis=-1, keepdims=True)
            normed = centered * lax.rsqrt(variance + epsilon)
            for part in range(width // 128):
                for k in range(step):
                    strided[part, pl.ds((i * step + k) * pitch, half), :] = normed[
                        k * half : (k + 1) * half, part * 128 : (part + 1) * 128
                    ]
            return carry

        lax.fori_loop(0, seqs // step, norm, 0, unroll=2)

        def move(k, carry):
            for n in range(COUNT):
                for part in range(width // 128):
                    gathered[q, base + k * COUNT + n, :, part * 128 : (part + 1) * 128] = strided[
                        part, pl.ds(k * COUNT + n, seqs, pitch), :
                    ].astype(jnp.bfloat16)
            return carry

        if turn == 0:
            for k in range(EARLY_PARTS):
                move(k, 0)
                cross_own(k).start()
            lax.fori_loop(EARLY_PARTS, half_parts, move, 0, unroll=2)
        else:
            lax.fori_loop(0, half_parts, move, 0, unroll=2)

    def start_twin(p, carry):
        direct(q, p, part_at(p)).start()
        return carry

    lax.fori_loop(0, parts, start_twin, 0)

    row = lax.broadcasted_iota(jnp.int32, (factor, pack * 128), 0)
    lane = lax.broadcasted_iota(jnp.int32, (factor, pack * 128), 1)
    chosen = jnp.where(lax.rem(lane, 128) == (lane // 128) * factor + row, 1.0, 0.0)
    placed[...] = lax.dot_general(
        wf_ref[factor:],
        chosen.astype(jnp.bfloat16),
        (((0,), (0,)), ((), ())),
        preferred_element_type=jnp.float32,
    ).astype(jnp.bfloat16)

    for g in range(residues // pack):
        total = mm(gathered[q, g * pack], placed[:, :128])
        for k in range(1, pack):
            total = total + mm(gathered[q, g * pack + k], placed[:, k * 128 : (k + 1) * 128])
        right_all[r, q, :, g * 128 : (g + 1) * 128] = total.astype(jnp.bfloat16)

    def factor_copy(kind, owner):
        target = (r, across) if kind == 0 else (r, twin)
        return send(right_all.at[r, owner], factor_send.at[kind], factor_recv.at[kind], target)

    def owner_of(piece, own=True):
        if own:
            return jnp.where(piece == 0, q, across)
        return jnp.where(piece == 0, twin, twin_across)

    def shifted(way, hop):
        return block_of(lax.rem(place + (blocks - hop if way == 0 else hop), blocks))

    def neighbour(way):
        return ((ahead if way == 0 else behind), q)

    def ring_copy(way, piece, hop):
        ref = right_all.at[shifted(way, hop), owner_of(piece)]
        sems = (ring_send.at[way, piece, hop], ring_recv.at[way, piece, hop])
        return send(ref, *sems, neighbour(way))

    def arrival(way, piece, hop):
        ref = right_all.at[shifted(way, hop + 1), owner_of(piece)]
        sems = (ring_send.at[way, piece, hop], ring_recv.at[way, piece, hop])
        return send(ref, *sems, neighbour(way))

    def share_copy(way, piece, hop, outward=True):
        ref = right_all.at[shifted(way, hop + 1), owner_of(piece, outward)]
        sems = (share_send.at[way, piece, hop], share_recv.at[way, piece, hop])
        return send(ref, *sems, (r, twin))

    def reach(way, piece):
        return jnp.where(piece == way, hops, hops - 1)

    def event(piece, hop):
        for way in range(2):

            @pl.when(hop < reach(way, piece))
            def _():
                arrival(way, piece, hop).wait_recv()

            @pl.when(hop + 1 < reach(way, piece))
            def _():
                ring_copy(way, piece, hop + 1).start()

            @pl.when(hop < reach(way, piece))
            def _():
                share_copy(way, piece, hop).start()

    factor_copy(0, q).start()
    for way in range(2):
        ring_copy(way, 0, 0).start()
    factor_copy(1, q).start()

    def start_across(p, carry):
        cross_own(p).start()
        return carry

    lax.fori_loop(EARLY_PARTS, parts, start_across, 0)

    def take_factors():
        factor_copy(0, across).wait_recv()
        for way in range(2):
            ring_copy(way, 1, 0).start()
        factor_copy(2, across).start()

    pair_rows[...] = wp_ref[...].astype(jnp.float32)
    spread[...] = jnp.zeros_like(spread)
    for c in range(factor):
        rows = pair_rows[c * factor : (c + 1) * factor, :].astype(jnp.bfloat16)
        for k in range(pack):
            start = (c * pack + k) * factor
            spread[start : start + factor, k * channels : (k + 1) * channels] = rows

    def take_across(p):
        cross(across, p, part_at(p)).wait_recv()
        relay(across, p, part_at(p)).start()

    def make_left():
        for i in range(own_rows):
            rows = gathered[:, q * own_rows + i].reshape(depth, width)
            value = mm_nt(wf_ref[:factor], rows)
            for k in range(depth // 128):
                left_rows[k, pl.ds(i, factor, own_rows), :] = value[:, k * 128 : (k + 1) * 128]
        for k in range(depth // 128):
            left_all[:, k * 128 : (k + 1) * 128] = left_rows[k].astype(jnp.bfloat16)

    jgroups = residues // pack

    def block_at(k):
        last = 2 * hops - 1
        hop = (k - 1) // 2 + 1
        even = jnp.where(lax.rem(k, 2) == 1, blocks - hop, hop)
        shift = jnp.where(k == 0, 0, jnp.where(k == last, hops, even))
        return block_of(lax.rem(place + shift, blocks))

    def pair_wait(k):
        last = 2 * hops - 1

        @pl.when(k == 0)
        def _():
            factor_copy(1, twin).wait_recv()
            factor_copy(2, twin_across).wait_recv()

        for way in range(2):

            @pl.when((k > 0) & (k < last) & (lax.rem(k + 1, 2) == way))
            def _():
                for piece in range(2):
                    share_copy(way, piece, (k - 1) // 2, False).wait_recv()

            @pl.when(k == last)
            def _():
                share_copy(way, way, hops - 1, False).wait_recv()

    def pair_first(k):
        block = block_at(k)
        value = mm(left_all[...], right_all[block].reshape(depth, residues * factor))
        base = pl.multiple_of(lax.rem(k, 2) * (jgroups * own_rows), jgroups * own_rows)
        for c in range(factor):
            for m in range(jgroups // 2):
                outer[
                    pl.ds(base + m * 2 * own_rows, 2 * own_rows), c * 128 : (c + 1) * 128
                ] = jnp.concatenate(
                    [
                        value[c * own_rows : (c + 1) * own_rows, g * 128 : (g + 1) * 128]
                        for g in (2 * m, 2 * m + 1)
                    ],
                    axis=0,
                ).astype(jnp.bfloat16)

    def pair_second(k):
        value = mm(outer[...], spread[...]) * scaling
        for t in range(2):
            for g in range(jgroups):
                start = (t * jgroups + g) * own_rows
                for j in range(pack):
                    products[t, pl.ds(g * pack + j, own_rows, pitch), :] = value[
                        start : start + own_rows, j * channels : (j + 1) * channels
                    ]
        for t in range(2):
            start = pl.multiple_of(block_at(k - 1 + t) * residues, residues)
            for i in range(own_rows):
                pair_ref[i, pl.ds(start, residues), :] = products[
                    t, pl.ds(i * pitch, residues), :
                ].astype(jnp.bfloat16)

    def pair_step(k):
        pair_wait(k)
        pair_first(k)

        @pl.when(lax.rem(k, 2) == 1)
        def _():
            pair_second(k)

    slots = (stages[: len(stages) // 2], stages[len(stages) // 2 :])
    chunks = HEADS * seqs // WIDE

    def residue_at(p, n):
        return part_at(lax.rem(p + parts + n // COUNT, parts)) * COUNT + n % COUNT

    def weigh_last(slot):
        weigh(slot[1], slot[4], chunks - 1, WIDE, seqs, slot[5][...], slot[6][0:1, :])

    def emit(slot, residue):
        update = finish_residue(slot[4], slot[3], wout_ref)
        for piece in range(width // 128):
            strided[piece, pl.ds(residue, seqs, pitch), :] = update[
                :, piece * 128 : (piece + 1) * 128
            ]

    def attend(slot, other, fresh, emitted):
        everything = gathered[:, fresh].reshape(depth, width) if fresh is not None else None
        held = [score(slot[0], slot[2], 0, WIDE)]
        weigh_last(other)
        for c in range(1, chunks):
            now = score(slot[0], slot[2], c, WIDE)
            if c == chunks - 1:
                slot[5][...], slot[6][0:1, :] = now
            if c == 1:
                emit(other, emitted)
                if fresh is not None:
                    prepare_queries(gathered[q, fresh], wq_ref, wg_ref, other[2], other[3])
            held.append(now)
            weigh(slot[1], slot[4], c - 1, WIDE, seqs, *held[c - 1])
            if c == 1 and fresh is not None:
                prepare_keys(everything, wkv_ref, other[0])
        if fresh is not None:
            prepare_values(everything, wkv_ref, other[1])

    take_across(0)
    events = 2 * hops
    loop_events = min((parts - FIRST_EVENT + 1) // 2, events)
    pair_start = half_parts
    loop_pairs = 1
    while (
        pair_start + loop_pairs < parts
        and FIRST_EVENT + 2 * ((loop_pairs - 1) // 2 * 2 + 1) <= pair_start + loop_pairs
    ):
        loop_pairs += 1

    def one_part(p, carry):
        part = part_at(p)

        @pl.when(p + 1 < parts)
        def _():
            take_across(p + 1)

        @pl.when(p == FIRST_EVENT - 1)
        def _():
            take_factors()

        number = p - FIRST_EVENT

        @pl.when((number >= 0) & (lax.rem(number, 2) == 0) & (number // 2 < loop_events))
        def _():
            event(lax.rem(number // 2, 2), number // 4)

        direct(twin, p, part).wait_recv()
        relay(twin_across, p, part).wait_recv()
        for n in range(COUNT):
            attend(slots[(n + 1) % 2], slots[n % 2], residue_at(p, n), residue_at(p, n - 2))

        @pl.when(p == pair_start - 1)
        def _():
            make_left()

        @pl.when((p >= pair_start) & (p - pair_start < loop_pairs))
        def _():
            pair_step(p - pair_start)

        return carry

    lax.fori_loop(0, parts, one_part, 0)

    def late(e, carry):
        event(lax.rem(e, 2), e // 2)
        return carry

    lax.fori_loop(loop_events, events, late, 0)
    attend(slots[1], slots[0], None, residue_at(parts - 1, COUNT - 2))
    weigh_last(slots[1])
    emit(slots[1], residue_at(parts - 1, COUNT - 1))

    def rest(k, carry):
        pair_step(k)
        return carry

    lax.fori_loop(loop_pairs, blocks, rest, 0)

    def finish(i, carry):
        for piece in range(width // 128):
            for k in range(step):
                o_ref[i * step + k, :, piece * 128 : (piece + 1) * 128] = strided[
                    piece, pl.ds((i * step + k) * pitch, residues), :
                ].astype(jnp.bfloat16)
        return carry

    lax.fori_loop(0, seqs // step, finish, 0)

    def drain(p, carry):
        cross_own(p).wait_send()
        direct(q, p, part_at(p)).wait_send()
        relay(across, p, part_at(p)).wait_send()
        return carry

    lax.fori_loop(0, parts, drain, 0)
    for kind, owner in ((0, q), (1, q), (2, across)):
        factor_copy(kind, owner).wait_send()
    for way in range(2):
        for piece in range(2):

            def drain_ring(hop, carry):
                ring_copy(way, piece, hop).wait_send()
                share_copy(way, piece, hop).wait_send()
                return carry

            lax.fori_loop(0, hops if way == piece else hops - 1, drain_ring, 0)


def export_kernel(update, pair, update_out, pair_out, sems):
    copies = []
    for k, (source, target) in enumerate(((update, update_out), (pair, pair_out))):
        rows = source.shape[0] // PIECES
        for n in range(PIECES):
            block = pl.ds(n * rows, rows)
            copies.append(pltpu.make_async_copy(source.at[block], target.at[block], sems.at[k, n]))
    for copy in copies:
        copy.start()
    for copy in copies:
        copy.wait()


def per_device(alignment, query_weight, w_keyval, w_gate, output_weight, w_factors, w_pair_out):
    seqs, residues, width = alignment.shape
    groups = lax.axis_size("seq")
    blocks = lax.axis_size("res")
    depth = seqs * groups
    factor = w_factors.shape[1] // 2
    hidden = HEADS * HC
    stage = [
        pltpu.VMEM((depth, hidden), jnp.bfloat16),
        pltpu.VMEM((hidden, depth), jnp.bfloat16),
        pltpu.VMEM((HEADS * seqs, hidden), jnp.bfloat16),
        pltpu.VMEM((seqs, hidden), jnp.float32),
        pltpu.VMEM((hidden, 128), jnp.float32),
        pltpu.VMEM((depth, WIDE), jnp.bfloat16),
        pltpu.VMEM((8, WIDE), jnp.float32),
    ]
    channels = w_pair_out.shape[1]
    own_rows = residues // groups
    parts = residues // COUNT
    hops = blocks // 2
    pack = 128 // factor
    pitch = residues + PITCH_PAD
    vmem = pl.BlockSpec(memory_space=pltpu.VMEM)
    dma = pltpu.SemaphoreType.DMA
    update, pair = pl.pallas_call(
        functools.partial(block_kernel, 1.0 / depth, blocks, groups),
        in_specs=[vmem] * 7,
        out_specs=[vmem] * 2,
        out_shape=[
            pltpu.VMEM((seqs, residues, width), jnp.bfloat16),
            pltpu.VMEM((own_rows, blocks * residues, channels), jnp.bfloat16),
        ],
        scratch_shapes=[
            pltpu.VMEM((groups, residues, seqs, width), jnp.bfloat16),
            pltpu.VMEM((width // 128, seqs * pitch, 128), jnp.float32),
            pltpu.VMEM((factor * factor, channels), jnp.float32),
            pltpu.VMEM((factor * 128, pack * channels), jnp.bfloat16),
            pltpu.VMEM((width, pack * 128), jnp.bfloat16),
            pltpu.VMEM((depth // 128, factor * own_rows, 128), jnp.float32),
            pltpu.VMEM((factor * own_rows, depth), jnp.bfloat16),
            pltpu.VMEM((blocks, groups, seqs, residues * factor), jnp.bfloat16),
            pltpu.VMEM((2 * residues // pack * own_rows, factor * 128), jnp.bfloat16),
            pltpu.VMEM((2, own_rows * pitch, channels), jnp.float32),
            dma((parts,)),
            dma((parts,)),
            dma((parts,)),
            dma((parts,)),
            dma((parts,)),
            dma((parts,)),
            dma((3,)),
            dma((3,)),
            dma((2, 2, hops)),
            dma((2, 2, hops)),
            dma((2, 2, hops)),
            dma((2, 2, hops)),
        ]
        + stage * 2,
        compiler_params=pltpu.CompilerParams(
            vmem_limit_bytes=52 * 1024 * 1024, collective_id=0, has_side_effects=True
        ),
        name="block",
    )(alignment, query_weight, w_keyval, w_gate, output_weight, w_factors.T, w_pair_out)
    anywhere = pl.BlockSpec(memory_space=pl.ANY)
    return pl.pallas_call(
        export_kernel,
        in_specs=[vmem] * 2,
        out_specs=[anywhere] * 2,
        out_shape=[
            jax.ShapeDtypeStruct(update.shape, update.dtype),
            jax.ShapeDtypeStruct(pair.shape, pair.dtype),
        ],
        scratch_shapes=[dma((2, PIECES))],
        compiler_params=pltpu.CompilerParams(vmem_limit_bytes=1024 * 1024),
        name="export",
    )(
        pltpu.with_memory_space_constraint(update, pltpu.MemorySpace.VMEM),
        pltpu.with_memory_space_constraint(pair, pltpu.MemorySpace.VMEM),
    )


def solution(mesh):
    in_specs = (P("seq", "res", None), P(), P(), P(), P(), P(), P())
    out_specs = (P("seq", "res", None), P(("res", "seq"), None, None))
    return jax.shard_map(
        per_device, mesh=mesh, in_specs=in_specs, out_specs=out_specs, check_vma=False
    )
```
